512 devices in a mesh: leaf: 128 (over y, z, core), top: 4 (over x).
Axes of the slice: x: 4, y: 8, z: 8, core: 2. Of those that a mesh axis runs over, the one named last changes fastest.
Arguments:
- charges: float32 [4, 16, 65536], P('top', None, 'leaf'), may hold values from -6 to 6
- leaf_basis: float32 [4, 1024, 64, 64], P('top', 'leaf'), may hold values from -0.75 to 0.75
- near_blocks: float32 [4, 1024, 3, 64, 64], P('top', 'leaf'), may hold values from -0.4375 to 0.4375
- near_list: int32 [4, 1024, 3], P('top', 'leaf'), may hold values from 0 to 8
- local_transfer: float32 [4, 1792, 64, 64], P('top', 'leaf'), may hold values from -0.5 to 0.5
- local_coupling: float32 [4, 1792, 3, 64, 64], P('top', 'leaf'), may hold values from -0.4375 to 0.4375
- coupling_list: int32 [4, 1792, 3], P('top', 'leaf'), may hold values from 0 to 23, as said below
- coarse_transfer: float32 [4, 7, 2, 64, 64], P('top'), may hold values from -0.5 to 0.5
- coarse_coupling: float32 [4, 5, 4, 64, 64], P('top'), may hold values from -0.4375 to 0.4375
- opposite_coupling: float32 [4, 64, 64], P('top'), may hold values from -0.75 to 0.75
- body_coupling: float32 [4, 3, 64, 64], P('top'), may hold values from -0.4375 to 0.4375
Outputs:
- potential: float32 [4, 16, 65536], P('top', None, 'leaf')
The draws below stay inside these ranges and needn't reach their ends.
Inputs may be any that keep to these rules, and one draw needn't show every extreme that they name: `coupling_list`: for a node of a device tier with m nodes per device the entry lies below 3 m; it names, in order, the m nodes of that tier on the previous device along the boundary, then this device's, then the next device's.
All inputs are finite; a program needn't handle non-finite values.
Results may differ from the reference program's by a relative error of at most 0.0001.
Values sent between devices are 32-bit elements; how exact they have to be, the bound alone decides.
A program may use at most 64 MiB of HBM per device.

```python
import jax
import jax.numpy as jnp
import numpy as np
from jax import lax

K = 64
RHS = 16
P_SIZE = 64
L0 = 8
NEAR = 4
LEVELS = 3
COARSE = 7
NODES = 14
LEAVES = 1024
N_LEAF = 128
N_TOP = 4


def draw_coupling_list(key, part):
    ranges = np.concatenate([np.full(L0 >> height, 3 * (L0 >> height)) for height in range(LEVELS)])
    limits = jnp.asarray(np.tile(ranges, N_LEAF), dtype=jnp.int32)
    return jax.random.randint(key, (N_TOP, N_LEAF * (2 * L0 - 2), 3), 0, limits[None, :, None], dtype=jnp.int32)


def set_ends(array, key, low, largest):
    extent = array.shape
    index_at = [jax.random.randint(jax.random.fold_in(key, axis), (), 0, extent[axis]) for axis in range(len(extent))]
    array = array.at[tuple(index_at)].set(low)
    longest = extent.index(max(extent))
    index_at[longest] = (index_at[longest] + 1) % extent[longest]
    return array.at[tuple(index_at)].set(largest)


def steps_of(key, dims, cuts, least, largest):
    factor_of = 1.0
    for axis_at, shards_of in cuts:
        steps = jax.random.uniform(jax.random.fold_in(jax.random.fold_in(key, 6), axis_at), (shards_of,), jnp.float32, least / len(cuts), largest / len(cuts))
        factor_of = factor_of * jnp.repeat(jnp.exp(steps), dims[axis_at] // shards_of).reshape((-1,) + (1,) * (len(dims) - 1 - axis_at))
    return factor_of


def bell_draw(own_key, extent, deviation, reach, shards=(), held_as=jnp.bfloat16):
    values = deviation * jax.random.normal(own_key, extent, jnp.float32)
    if shards:
        values = values * steps_of(own_key, extent, shards, -0.22, 0.18)
    return jnp.clip(values, -reach, reach).astype(held_as)


def setup_inputs(seed: int = 0) -> dict:
    key_list = jax.random.split(jax.random.key(seed), 12)
    return {
        "charges": bell_draw(key_list[0], (N_TOP, RHS, LEAVES * P_SIZE), 1.0, 6.0, ((0, 4), (2, 128)), jnp.float32),
        "leaf_basis": bell_draw(key_list[1], (N_TOP, LEAVES, P_SIZE, K), P_SIZE ** -0.5, 0.75, ((0, 4), (1, 128)), jnp.float32),
        "near_blocks": bell_draw(key_list[2], (N_TOP, LEAVES, 3, P_SIZE, P_SIZE), (3 * P_SIZE) ** -0.5, 0.4375, ((0, 4), (1, 128)), jnp.float32),
        "near_list": set_ends(jax.random.randint(key_list[3], (N_TOP, LEAVES, 3), 0, 2 * NEAR + 1), jax.random.fold_in(key_list[3], 1), 0, 2 * NEAR).astype(jnp.int32),
        "local_transfer": bell_draw(key_list[4], (N_TOP, N_LEAF * NODES, K, K), (2 * K) ** -0.5, 0.5, ((0, 4), (1, 128)), jnp.float32),
        "local_coupling": bell_draw(key_list[5], (N_TOP, N_LEAF * NODES, 3, K, K), (3 * K) ** -0.5, 0.4375, ((0, 4), (1, 128)), jnp.float32),
        "coupling_list": draw_coupling_list(jax.random.fold_in(key_list[11], 71), 0),
        "coarse_transfer": bell_draw(key_list[7], (N_TOP, COARSE, 2, K, K), (2 * K) ** -0.5, 0.5, ((0, 4),), jnp.float32),
        "coarse_coupling": bell_draw(key_list[8], (N_TOP, COARSE - 2, 4, K, K), (3 * K) ** -0.5, 0.4375, ((0, 4),), jnp.float32),
        "opposite_coupling": bell_draw(key_list[9], (N_TOP, K, K), K ** -0.5, 0.75, ((0, 4),), jnp.float32),
        "body_coupling": bell_draw(key_list[10], (N_TOP, N_TOP - 1, K, K), ((N_TOP - 1) * K) ** -0.5, 0.4375, ((0, 4),), jnp.float32),
    }


HIGH = lax.Precision.HIGHEST
OFFSETS = (-3, -2, 2, 3)


def upward(charges, leaf_basis, local_transfer):
    rhs = charges.shape[0]
    leaves = leaf_basis.shape[0]
    blocks = charges.reshape(rhs, leaves, P_SIZE)
    coeffs = [jnp.einsum('rnp,npk->rnk', blocks, leaf_basis, precision=HIGH)]
    nodes = local_transfer.reshape(N_LEAF, 2 * L0 - 2, K, K)
    for height in range(LEVELS):
        members = L0 >> height
        first = 2 * L0 - 2 * members
        mats = nodes[:, first:first + members].reshape(N_LEAF * members, K, K)
        moved = jnp.einsum('rnk,nkj->rnj', coeffs[-1], mats, precision=HIGH)
        coeffs.append(moved[:, 0::2] + moved[:, 1::2])
    return coeffs


def coarse_up(device_coeff, coarse_transfer):
    tiers = [device_coeff]
    for height in range(COARSE):
        below = tiers[-1]
        left = jnp.einsum('rnk,kj->rnj', below[:, 0::2], coarse_transfer[height, 0], precision=HIGH)
        right = jnp.einsum('rnk,kj->rnj', below[:, 1::2], coarse_transfer[height, 1], precision=HIGH)
        tiers.append(left + right)
    return tiers


def coarse_couple(tier, height, coarse_coupling, opposite_coupling):
    members = tier.shape[1]
    parity = jnp.arange(members, dtype=jnp.int32) % 2
    if height <= COARSE - 3:
        total = jnp.zeros_like(tier)
        for which, offset in enumerate(OFFSETS):
            moved = jnp.einsum('rnk,kj->rnj', jnp.roll(tier, -offset, axis=1), coarse_coupling[height, which], precision=HIGH)
            if offset == -3:
                keep = parity == 1
            elif offset == 3:
                keep = parity == 0
            else:
                keep = parity >= 0
            total = total + jnp.where(keep[None, :, None], moved, 0.0)
        return total
    if height == COARSE - 2:
        return jnp.einsum('rnk,kj->rnj', jnp.roll(tier, -2, axis=1), opposite_coupling, precision=HIGH)
    return jnp.zeros_like(tier)


def coarse_down(tiers, body_local, coarse_transfer, coarse_coupling, opposite_coupling):
    local = body_local
    for height in range(COARSE - 1, -1, -1):
        tier = tiers[height]
        members = tier.shape[1]
        parent = jnp.repeat(local, 2, axis=1)
        side = jnp.arange(members, dtype=jnp.int32) % 2
        mats = jnp.where(side[:, None, None] == 0, coarse_transfer[height, 0][None], coarse_transfer[height, 1][None])
        down = jnp.einsum('rnj,nkj->rnk', parent, mats, precision=HIGH)
        local = coarse_couple(tier, height, coarse_coupling, opposite_coupling) + down
    return local


def local_down(coeffs, device_local, local_transfer, local_coupling, coupling_list):
    nodes_t = local_transfer.reshape(N_LEAF, 2 * L0 - 2, K, K)
    nodes_s = local_coupling.reshape(N_LEAF, 2 * L0 - 2, 3, K, K)
    lists = coupling_list.reshape(N_LEAF, 2 * L0 - 2, 3)
    local = device_local
    for height in range(LEVELS - 1, -1, -1):
        members = L0 >> height
        first = 2 * L0 - 2 * members
        whole = N_LEAF * members
        window = lists[:, first:first + members]
        base = (jnp.arange(N_LEAF, dtype=jnp.int32) * members - members)[:, None, None]
        source = ((base + window) % whole).astype(jnp.int32).reshape(whole, 3)
        picked = coeffs[height][:, source]
        mats = nodes_s[:, first:first + members].reshape(whole, 3, K, K)
        coupled = jnp.einsum('rnsk,nskj->rnj', picked, mats, precision=HIGH)
        parent = jnp.repeat(local, 2, axis=1)
        trans = nodes_t[:, first:first + members].reshape(whole, K, K)
        down = jnp.einsum('rnj,nkj->rnk', parent, trans, precision=HIGH)
        local = coupled + down
    return local


def reference(charges, leaf_basis, near_blocks, near_list, local_transfer, local_coupling, coupling_list, coarse_transfer, coarse_coupling, opposite_coupling, body_coupling):
    ups = []
    tops = []
    for body_index in range(N_TOP):
        coeffs = upward(charges[body_index], leaf_basis[body_index], local_transfer[body_index])
        tiers = coarse_up(coeffs[-1], coarse_transfer[body_index])
        ups.append((coeffs, tiers))
        tops.append(tiers[-1])
    results = []
    for body_index in range(N_TOP):
        coeffs, tiers = ups[body_index]
        rhs = charges.shape[1]
        body_local = jnp.zeros((rhs, 1, K), jnp.float32)
        for which in range(N_TOP - 1):
            source = tops[(body_index + 1 + which) % N_TOP]
            body_local = body_local + jnp.einsum('rnk,kj->rnj', source, body_coupling[body_index, which], precision=HIGH)
        device_local = coarse_down(tiers, body_local, coarse_transfer[body_index], coarse_coupling[body_index], opposite_coupling[body_index])
        leaf_local = local_down(coeffs, device_local, local_transfer[body_index], local_coupling[body_index], coupling_list[body_index])
        far = jnp.einsum('rnk,npk->rnp', leaf_local, leaf_basis[body_index], precision=HIGH)
        blocks = charges[body_index].reshape(rhs, LEAVES, P_SIZE)
        source = ((jnp.arange(LEAVES, dtype=jnp.int32)[:, None] + near_list[body_index] - NEAR) % LEAVES).astype(jnp.int32)
        picked = blocks[:, source]
        near = jnp.einsum('rnsq,nsqp->rnp', picked, near_blocks[body_index], precision=HIGH)
        results.append((far + near).reshape(rhs, LEAVES * P_SIZE))
    return jnp.stack(results)
```

```python
import functools

import jax
import jax.numpy as jnp
from jax import lax
from jax.experimental import pallas as pl
from jax.experimental.pallas import tpu as pltpu
from jax.sharding import PartitionSpec as P

HIGH = lax.Precision.HIGH
MESH = pl.DeviceIdType.MESH
F32 = jnp.float32
K = 64
RHS = 16
NEAR = 4
L0 = 8
NODES = 14
FIRST = (0, 8, 12)


def mm(x, w):
    return lax.dot_general(x, w, (((1,), (0,)), ((), ())), precision=HIGH, preferred_element_type=F32)


def mm_t(x, w):
    return lax.dot_general(x, w, (((1,), (1,)), ((), ())), precision=HIGH, preferred_element_type=F32)


def bmm(x, w):
    return lax.dot_general(x, w, (((2,), (1,)), ((0,), (0,))), precision=HIGH, preferred_element_type=F32)


def bmm_t(x, w):
    return lax.dot_general(x, w, (((2,), (2,)), ((0,), (0,))), precision=HIGH, preferred_element_type=F32)


def pack(x):
    h = RHS // 2
    if x.ndim == 2:
        return jnp.concatenate([x[:h], x[h:]], axis=1)
    return jnp.concatenate([x[:, :h], x[:, h:]], axis=2)


def unpack(x):
    if x.ndim == 2:
        return jnp.concatenate([x[:, :K], x[:, K:]], axis=0)
    return jnp.concatenate([x[:, :, :K], x[:, :, K:]], axis=1)


def kernel(
    Y, Z, X,
    near_list_hbm, coupling_list_hbm,
    charges_hbm, basis_hbm, near_hbm, transfer_hbm, coupling_hbm,
    ct_hbm, cc_hbm, opp_hbm, bc_hbm,
    out_ref,
    charges, basis, near, transfer, coupling, ct, cc, opp, bc, near_list, coupling_list, path_mats,
    qbuf, rows, u4buf, xsrc, xbuf, gbuf, sbuf, tiers, leaves, pg_hi, pg_lo, acc,
    load_sem, ready_sem, send_sem, recv_sem,
):
    ZL = Z.bit_length() - 1
    YL = Y.bit_length() - 1
    R = ZL + 1
    COARSE = R + YL
    W = 2 * Z
    N = Y * W
    START = [2 * W - (2 * W >> c) for c in range(R)]
    TILES = 2 * W - 2

    i = lax.axis_index("leaf")
    b = lax.axis_index("top")
    k = i % 2
    z = (i // 2) % Z
    y = i // W
    j = i % W
    side = [(i // (1 << c)) % 2 for c in range(COARSE)]

    def dev(leaf, top):
        return {"leaf": leaf, "top": top}

    order = []
    for a in range(Z // 2, 0, -1):
        order.append(a)
        if Z - a != a:
            order.append(Z - a)
    order_y = []
    for a in range(Y // 2, 0, -1):
        order_y.append(a)
        if Y - a != a:
            order_y.append(Y - a)
    order_x = sorted(range(1, X), key=lambda a: -min(a, X - a))
    near_first = lambda count: sorted(range(count), key=lambda a: min(a, count - a))
    order_xy = [(x, r) for r in near_first(Y) for x in near_first(X)]
    order_xy.sort(key=lambda t: min(t[0], X - t[0]) + min(t[1], Y - t[1]))
    row_offsets = [(dz, dk) for dz in order for dk in (0, 1)] + [(0, 1)]

    def row_dev(dz, dk):
        return dev(y * W + ((z + dz) % Z) * 2 + (k + dk) % 2, b)

    def y_dev(dy):
        return dev(((y + dy) % Y) * W + j, b)

    def x_dev(dx):
        return dev(i, (b + dx) % X)

    nxt = dev((i + 1) % N, b)
    prv = dev((i + N - 1) % N, b)

    early = [(charges_hbm, charges), (basis_hbm, basis), (transfer_hbm, transfer)]
    early += [(ct_hbm.at[0, c, side[c]], path_mats.at[c]) for c in range(R)]
    later = [
        (ct_hbm, ct), (bc_hbm, bc), (opp_hbm, opp), (cc_hbm, cc), (near_hbm, near), (coupling_hbm, coupling),
        (near_list_hbm, near_list), (coupling_list_hbm, coupling_list),
    ]
    loads = [pltpu.make_async_copy(src, dst, load_sem.at[n]) for n, (src, dst) in enumerate(early + later)]
    early, later = loads[:len(early)], loads[len(early):]
    for load in early:
        load.start()

    def await_all(sem, ref):
        pltpu.make_async_copy(ref, ref, sem).wait()

    barrier = pltpu.get_barrier_semaphore()
    partners = [(min(dz, Z - dz), row_dev(dz, dk)) for dz, dk in row_offsets] + [(min(a, Y - a), y_dev(a)) for a in order_y]
    partners += [(min(a, X - a), x_dev(a)) for a in order_x] + [(1, nxt), (1, prv)]
    partners = [p for _, p in sorted(partners, key=lambda t: -t[0])]
    for p in partners:
        pl.semaphore_signal(barrier, inc=1, device_id=p, device_id_type=MESH)

    for load in early[:2]:
        load.wait()

    dens = charges[0]
    blocks = jnp.stack([dens[:, K * l:K * (l + 1)] for l in range(L0)], axis=0)
    leaves[NEAR:NEAR + L0] = pack(blocks)
    c0 = bmm(blocks, basis[0])
    for load in early[2:]:
        load.wait()
    for load in later:
        load.start()
    parts = [path_mats[c] for c in range(R)]
    while len(parts) > 1:
        parts = [mm(*parts[n:n + 2]) if n + 1 < len(parts) else parts[n] for n in range(0, len(parts), 2)]
    path = parts[0]
    up = [c0]
    for h in range(2):
        m = L0 >> h
        moved = bmm(up[-1], transfer[0, FIRST[h]:FIRST[h] + m])
        moved = moved.reshape(m // 2, 2, RHS, K)
        up.append(moved[:, 0] + moved[:, 1])
    last = [transfer[0, FIRST[2] + n] for n in range(2)]
    q_own = mm(up[2][0], mm(last[0], path)) + mm(up[2][1], mm(last[1], path))
    own = mm(up[2][0], last[0]) + mm(up[2][1], last[1])

    qbuf[j] = pack(q_own)
    rows[j] = pack(own)
    tiers[NODES:NODES + L0] = pack(up[0])
    tiers[NODES + 8:NODES + 12] = pack(up[1])
    tiers[NODES + 12:NODES + 14] = pack(up[2])

    pl.semaphore_wait(barrier, len(partners))
    for a in order_x:
        pl.semaphore_signal(ready_sem, inc=1, device_id=x_dev(a), device_id_type=MESH)

    def send_to_row(ref, at):
        for to_z in near_first(Z):
            for to_k in (1, 0):
                @pl.when((z != to_z) | (k != to_k))
                def _():
                    pltpu.make_async_remote_copy(
                        src_ref=ref.at[j], dst_ref=ref.at[j], send_sem=send_sem.at[at], recv_sem=recv_sem.at[at],
                        device_id=dev(y * W + to_z * 2 + to_k, b), device_id_type=MESH).start()

    send_to_row(qbuf, 0)

    square = (K, K)
    unit = (lax.broadcasted_iota(jnp.int32, square, 0) == lax.broadcasted_iota(jnp.int32, square, 1)).astype(F32)
    down = jnp.concatenate([unit, path.T], axis=0)[None]
    for h in (2, 1, 0):
        m = L0 >> h
        down = jnp.broadcast_to(down[:, None], (m // 2, 2, 2 * K, K)).reshape(m, 2 * K, K)
        down = bmm_t(down, transfer[0, FIRST[h]:FIRST[h] + m])
    down = bmm_t(down, basis[0])
    for l in range(0, L0, 2):
        joined = jnp.concatenate([down[l], down[l + 1]], axis=1)
        hi = joined.astype(jnp.bfloat16)
        pg_hi[:, K * l:K * (l + 2)] = hi
        pg_lo[:, K * l:K * (l + 2)] = (joined - hi.astype(F32)).astype(jnp.bfloat16)

    send_to_row(rows, 1)
    for n, (src, dst, to) in enumerate((
        (leaves.at[pl.ds(L0, NEAR)], leaves.at[pl.ds(0, NEAR)], nxt),
        (leaves.at[pl.ds(NEAR, NEAR)], leaves.at[pl.ds(NEAR + L0, NEAR)], prv),
        (tiers.at[pl.ds(NODES, NODES)], tiers.at[pl.ds(0, NODES)], nxt),
        (tiers.at[pl.ds(NODES, NODES)], tiers.at[pl.ds(2 * NODES, NODES)], prv),
    )):
        at = 2 + n // 2
        copy = pltpu.make_async_remote_copy(
            src_ref=src, dst_ref=dst, send_sem=send_sem.at[at], recv_sem=recv_sem.at[at],
            device_id=to, device_id_type=MESH)
        copy.start()

    for load in later:
        load.wait()

    path_y = ct[0, R, side[R]]
    for c in range(R + 1, COARSE):
        path_y = mm(path_y, ct[0, c, side[c]])
    for s in range(X - 1):
        sbuf[s] = mm_t(bc[0, s], path_y)
    if R == COARSE - 3:
        for n in range(2):
            sbuf[X - 1 + n] = mm_t(mm(ct[0, R, n], opp[0]), ct[0, R, side[R]])


    await_all(recv_sem.at[0], qbuf.at[pl.ds(1, W - 1)])
    total = qbuf[0]
    for n in range(1, W):
        total = total + qbuf[n]
    u_row = unpack(total)
    xsrc[...] = pack(mm(u_row, path_y))
    u4buf[y] = total
    pl.semaphore_wait(ready_sem, len(order_x))
    for to_x, to_y in order_xy:
        @pl.when(b != to_x)
        def _():
            pltpu.make_async_remote_copy(
                src_ref=xsrc, dst_ref=xbuf.at[((b - to_x + X) % X) * Y + y], send_sem=send_sem.at[5],
                recv_sem=recv_sem.at[5], device_id=dev(to_y * W + j, to_x), device_id_type=MESH).start()

        @pl.when((b == to_x) & (y != to_y))
        def _():
            pltpu.make_async_remote_copy(
                src_ref=u4buf.at[y], dst_ref=u4buf.at[y], send_sem=send_sem.at[4], recv_sem=recv_sem.at[4],
                device_id=dev(to_y * W + j, b), device_id_type=MESH).start()

    await_all(recv_sem.at[1], rows.at[pl.ds(0, W - 1)])
    tier = unpack(rows[0:W])
    for c in range(R - 1):
        m = W >> c
        pairs = tier.reshape(m // 2, 2, RHS, K)
        left = mm(pairs[:, 0].reshape(m // 2 * RHS, K), ct[0, c, 0])
        right = mm(pairs[:, 1].reshape(m // 2 * RHS, K), ct[0, c, 1])
        tier = (left + right).reshape(m // 2, RHS, K)
        rows[START[c + 1]:START[c + 1] + m // 2] = pack(tier)

    given = None
    for c in range(R - 1, -1, -1):
        m = W >> c
        if given is None:
            given = [jnp.zeros((RHS, K), F32)] * 3
        else:
            moved = mm_t(jnp.concatenate(given, axis=0), ct[0, c, side[c]])
            given = [moved[RHS * n:RHS * (n + 1)] for n in range(3)]
        third = 3 - 6 * side[c]
        for offset, slot in ((-2, 1), (2, 2), (third, 3 - 3 * side[c])):
            at = j // (1 << c) + offset
            term = mm(unpack(rows[START[c] + (at + m) % m]), cc[0, c, slot])
            for n, keep in enumerate((at >= m, (at >= 0) & (at < m), at < 0)):
                given[n] = given[n] + jnp.where(keep, term, 0.0)
    v_own = given[1]
    gbuf[0] = pack(given[0])
    gbuf[1] = pack(given[2])
    for n, to in enumerate((y_dev(Y - 1), y_dev(1))):
        copy = pltpu.make_async_remote_copy(
            src_ref=gbuf.at[n], dst_ref=gbuf.at[2 + n], send_sem=send_sem.at[6], recv_sem=recv_sem.at[6],
            device_id=to, device_id_type=MESH)
        copy.start()

    await_all(recv_sem.at[2], leaves.at[pl.ds(0, 2 * NEAR)])
    for l in range(L0):
        total = None
        for s in range(3):
            term = mm(unpack(leaves[near_list[s, 0, l] + l]), near[0, l, s])
            total = term if total is None else total + term
        acc[l] = total

    await_all(recv_sem.at[3], tiers.at[pl.ds(0, 2 * NODES)])
    coupled = []
    for h in range(3):
        m = L0 >> h
        terms = []
        for n in range(m):
            node = FIRST[h] + n
            total = None
            for s in range(3):
                e = coupling_list[s, 0, node]
                where = (e // m) * NODES + FIRST[h] + e % m
                term = mm(unpack(tiers[where]), coupling[0, node, s])
                total = term if total is None else total + term
            terms.append(total)
        coupled.append(jnp.stack(terms, axis=0))

    local = coupled[2]
    for h in (1, 0):
        m = L0 >> h
        local = jnp.broadcast_to(local[:, None], (m // 2, 2, RHS, K)).reshape(m, RHS, K)
        local = coupled[h] + bmm_t(local, transfer[0, FIRST[h]:FIRST[h] + m])
    field = bmm_t(local, basis[0]) + acc[...]
    for l in range(0, L0, 2):
        out_ref[0, :, K * l:K * (l + 2)] = jnp.concatenate([field[l], field[l + 1]], axis=1)

    await_all(recv_sem.at[6], gbuf.at[pl.ds(2, 2)])
    v_own = v_own + unpack(gbuf[2]) + unpack(gbuf[3])

    await_all(recv_sem.at[4], u4buf.at[pl.ds(0, Y - 1)])
    if R == COARSE - 3:
        third = 3 - 6 * side[R]
        row = None
        for offset, slot in ((-2, 1), (2, 2), (third, 3 - 3 * side[R])):
            term = mm(unpack(u4buf[(y + offset + Y) % Y]), cc[0, R, slot])
            row = term if row is None else row + term
        pair = 2 * ((y // 2 + 2) % (Y // 2))
        row = row + mm(unpack(u4buf[pair]), sbuf[X - 1]) + mm(unpack(u4buf[pair + 1]), sbuf[X])
    else:
        row = mm(unpack(u4buf[(y + 2) % Y]), opp[0])

    await_all(recv_sem.at[5], xbuf.at[pl.ds(Y, (X - 1) * Y)])
    for s in range(X - 1):
        total = xbuf[(s + 1) * Y]
        for n in range(1, Y):
            total = total + xbuf[(s + 1) * Y + n]
        row = row + mm(unpack(total), sbuf[s])
    late = jnp.concatenate([v_own, row], axis=1)
    hi = late.astype(jnp.bfloat16)
    lo = (late - hi.astype(F32)).astype(jnp.bfloat16)
    both = jnp.dot(jnp.concatenate([hi, lo], axis=0), pg_hi[...], preferred_element_type=F32)
    out_ref[0] = out_ref[0] + (both[:RHS] + both[RHS:] + jnp.dot(hi, pg_lo[...], preferred_element_type=F32))

    await_all(send_sem.at[0], qbuf.at[pl.ds(1, W - 1)])
    await_all(send_sem.at[1], rows.at[pl.ds(0, W - 1)])
    await_all(send_sem.at[2], leaves.at[pl.ds(0, 2 * NEAR)])
    await_all(send_sem.at[3], tiers.at[pl.ds(0, 2 * NODES)])
    await_all(send_sem.at[4], u4buf.at[pl.ds(0, Y - 1)])
    await_all(send_sem.at[5], xbuf.at[pl.ds(Y, (X - 1) * Y)])
    await_all(send_sem.at[6], gbuf.at[pl.ds(2, 2)])


def per_device(Y, Z, X, charges, leaf_basis, near_blocks, near_list, local_transfer, local_coupling, coupling_list,
               coarse_transfer, coarse_coupling, opposite_coupling, body_coupling):
    near_at = near_list.transpose(2, 0, 1)
    coupling_at = coupling_list.transpose(2, 0, 1)
    W = 2 * Z
    R = Z.bit_length()
    dma = pltpu.SemaphoreType.DMA
    vm = lambda *shape: pltpu.VMEM(shape, F32)
    operands = (charges, leaf_basis, near_blocks, local_transfer, local_coupling,
                coarse_transfer, coarse_coupling, opposite_coupling, body_coupling)
    return pl.pallas_call(
        functools.partial(kernel, Y, Z, X),
        out_shape=pltpu.VMEM(charges.shape, F32),
        in_specs=[pl.BlockSpec(memory_space=pltpu.HBM)] * 11,
        out_specs=pl.BlockSpec(memory_space=pltpu.VMEM),
        scratch_shapes=[
            *[vm(*a.shape) for a in operands],
            pltpu.SMEM(near_at.shape, jnp.int32), pltpu.SMEM(coupling_at.shape, jnp.int32),
            vm(R, K, K),
            vm(W, 8, 128), vm(2 * W - 2, 8, 128), vm(Y, 8, 128), vm(8, 128), vm(X * Y, 8, 128), vm(4, 8, 128), vm(X + 1, K, K),
            vm(3 * NODES, 8, 128), vm(L0 + 2 * NEAR, 8, 128),
            pltpu.VMEM((2 * K, L0 * K), jnp.bfloat16), pltpu.VMEM((2 * K, L0 * K), jnp.bfloat16), vm(L0, RHS, K),
            dma((11 + R,)), pltpu.SemaphoreType.REGULAR, dma((7,)), dma((7,)),
        ],
        compiler_params=pltpu.CompilerParams(collective_id=0, has_side_effects=True),
    )(near_at, coupling_at, *operands)


def solution(mesh):
    n = mesh.shape["leaf"]
    Z = 8 if n == 128 else 2
    Y = n // (2 * Z)
    X = mesh.shape["top"]
    in_specs = (
        P("top", None, "leaf"),
        P("top", "leaf", None, None),
        P("top", "leaf", None, None, None),
        P("top", "leaf", None),
        P("top", "leaf", None, None),
        P("top", "leaf", None, None, None),
        P("top", "leaf", None),
        P("top", None, None, None, None),
        P("top", None, None, None, None),
        P("top", None, None),
        P("top", None, None, None),
    )
    return jax.shard_map(
        functools.partial(per_device, Y, Z, X), mesh=mesh, in_specs=in_specs,
        out_specs=P("top", None, "leaf"), check_vma=False
    )
```

```python
import functools

import jax
import jax.numpy as jnp
from jax import lax
from jax.experimental import pallas as pl
from jax.experimental.pallas import tpu as pltpu
from jax.sharding import PartitionSpec as P

HIGH = lax.Precision.HIGH
MESH = pl.DeviceIdType.MESH
F32 = jnp.float32
K = 64
RHS = 16
NEAR = 4
L0 = 8
NODES = 14
FIRST = (0, 8, 12)


def split(a):
    hi = a.astype(jnp.bfloat16)
    return hi, (a - hi.astype(F32)).astype(jnp.bfloat16)


def product(x, w, dims):
    rows = x.ndim - 2
    xh, xl = split(x)
    wh, wl = w if isinstance(w, tuple) else split(w)
    dot = functools.partial(lax.dot_general, dimension_numbers=dims, preferred_element_type=F32)
    both = dot(jnp.concatenate([xh, xl], axis=rows), wh)
    m = x.shape[rows]
    return lax.slice_in_dim(both, 0, m, axis=rows) + (lax.slice_in_dim(both, m, 2 * m, axis=rows) + dot(xh, wl))


def mm(x, w):
    return product(x, w, (((1,), (0,)), ((), ())))


def mm_t(x, w):
    return product(x, w, (((1,), (1,)), ((), ())))


def bmm(x, w):
    return product(x, w, (((2,), (1,)), ((0,), (0,))))


def bmm_t(x, w):
    return product(x, w, (((2,), (2,)), ((0,), (0,))))


def pack(x):
    h = RHS // 2
    if x.ndim == 2:
        return jnp.concatenate([x[:h], x[h:]], axis=1)
    return jnp.concatenate([x[:, :h], x[:, h:]], axis=2)


def unpack(x):
    if x.ndim == 2:
        return jnp.concatenate([x[:, :K], x[:, K:]], axis=0)
    return jnp.concatenate([x[:, :, :K], x[:, :, K:]], axis=1)


def kernel(
    Y, Z, X,
    near_list_hbm, coupling_list_hbm,
    charges_hbm, basis_hbm, near_hbm, transfer_hbm, coupling_hbm,
    ct_hbm, cc_hbm, opp_hbm, bc_hbm,
    out_ref,
    charges, basis, near, transfer, coupling, ct, cc, opp, bc, near_list, coupling_list,
    qbuf, rows, u4buf, xsrc, xbuf, gbuf, sbuf, tiers, leaves, pg_hi, pg_lo, far_hi, far_lo, acc,
    vbuf, load_sem, state, send_sem, recv_sem,
):
    ZL = Z.bit_length() - 1
    YL = Y.bit_length() - 1
    R = ZL + 1
    COARSE = R + YL
    W = 2 * Z
    N = Y * W
    START = [2 * W - (2 * W >> c) for c in range(R)]
    TILES = 2 * W - 2

    i = lax.axis_index("leaf")
    b = lax.axis_index("top")
    k = i % 2
    z = (i // 2) % Z
    y = i // W
    j = i % W
    half = Z // 2
    first = z < half
    second = z >= half
    origin = (z == 0) & (k == 0)
    final = (z == Z - 1) & (k == 1)
    one = lambda flag: jnp.where(flag, 1, 0)
    side = [(i // (1 << c)) % 2 for c in range(COARSE)]

    def dev(leaf, top):
        return {"leaf": leaf, "top": top}

    order = []
    for a in range(Z // 2, 0, -1):
        order.append(a)
        if Z - a != a:
            order.append(Z - a)
    order_y = []
    for a in range(Y // 2, 0, -1):
        order_y.append(a)
        if Y - a != a:
            order_y.append(Y - a)
    order_x = sorted(range(1, X), key=lambda a: -min(a, X - a))
    near_first = lambda count: sorted(range(count), key=lambda a: min(a, count - a))
    order_xy = [(x, r) for r in near_first(Y) for x in near_first(X)]
    order_xy.sort(key=lambda t: min(t[0], X - t[0]) + min(t[1], Y - t[1]))
    row_offsets = [(dz, dk) for dz in order for dk in (0, 1)] + [(0, 1)]

    def row_dev(dz, dk):
        return dev(y * W + ((z + dz) % Z) * 2 + (k + dk) % 2, b)

    def y_dev(dy):
        return dev(((y + dy) % Y) * W + j, b)

    def x_dev(dx):
        return dev(i, (b + dx) % X)

    nxt = dev((i + 1) % N, b)
    prv = dev((i + N - 1) % N, b)

    early = [(charges_hbm, charges), (basis_hbm, basis), (transfer_hbm.at[0], transfer.at[0, pl.ds(0, NODES)])]
    later = [
        (ct_hbm, ct), (bc_hbm, bc), (opp_hbm, opp), (cc_hbm, cc), (near_hbm, near), (coupling_hbm, coupling),
        (near_list_hbm, near_list), (coupling_list_hbm, coupling_list),
    ]
    loads = [pltpu.make_async_copy(src, dst, load_sem.at[n]) for n, (src, dst) in enumerate(early + later)]
    early, later = loads[:len(early)], loads[len(early):]
    for load in early:
        load.start()
    for c in range(R):
        pltpu.make_async_copy(ct_hbm.at[0, c, side[c]], transfer.at[0, NODES + c], load_sem.at[2]).start()

    def await_all(sem, ref):
        pltpu.make_async_copy(ref, ref, sem).wait()

    barrier = pltpu.get_barrier_semaphore()
    partners = [(min(dz, Z - dz), row_dev(dz, dk)) for dz, dk in row_offsets] + [(min(a, Y - a), y_dev(a)) for a in order_y]
    partners += [(min(a, X - a), x_dev(a)) for a in order_x]
    partners = [p for _, p in sorted(partners, key=lambda t: -t[0])]

    @pl.when(first)
    def _():
        for p in partners:
            pl.semaphore_signal(barrier, inc=1, device_id=p, device_id_type=MESH)

    @pl.when(origin)
    def _():
        pl.semaphore_signal(barrier, inc=1, device_id=prv, device_id_type=MESH)

    for load in early[:2]:
        load.wait()

    dens = charges[0]
    blocks = jnp.stack([dens[:, K * l:K * (l + 1)] for l in range(L0)], axis=0)
    leaves[NEAR:NEAR + L0] = pack(blocks)
    c0 = bmm(blocks, basis[0])
    pltpu.make_async_copy(transfer, transfer, load_sem.at[2]).wait()
    for load in later:
        load.start()
    parts = [transfer[0, NODES + c] for c in range(R)]
    while len(parts) > 1:
        parts = [mm(*parts[n:n + 2]) if n + 1 < len(parts) else parts[n] for n in range(0, len(parts), 2)]
    path = parts[0]
    up = [c0]
    for h in range(2):
        m = L0 >> h
        moved = bmm(up[-1], transfer[0, FIRST[h]:FIRST[h] + m])
        moved = moved.reshape(m // 2, 2, RHS, K)
        up.append(moved[:, 0] + moved[:, 1])
    last = [transfer[0, FIRST[2] + n] for n in range(2)]
    q_own = mm(up[2][0], mm(last[0], path)) + mm(up[2][1], mm(last[1], path))
    own = mm(up[2][0], last[0]) + mm(up[2][1], last[1])

    qbuf[j] = pack(q_own)
    rows[j] = pack(own)
    tiers[NODES:NODES + L0] = pack(up[0])
    tiers[NODES + 8:NODES + 12] = pack(up[1])
    tiers[NODES + 12:NODES + 14] = pack(up[2])

    pl.semaphore_wait(barrier, 2 * half + one(final) + one(first) * (len(order_y) + len(order_x) - 1))

    @pl.when(first)
    def _():
        for a in order_x:
            pl.semaphore_signal(state.at[0], inc=1, device_id=x_dev(a), device_id_type=MESH)

    @pl.when(second)
    def _():
        for to_z in range(half):
            for to_k in range(2):
                pl.semaphore_signal(state.at[1], inc=1, device_id=dev(y * W + to_z * 2 + to_k, b), device_id_type=MESH)

    @pl.when(final)
    def _():
        pl.semaphore_signal(state.at[1], inc=1, device_id=nxt, device_id_type=MESH)

    mate = dev(y * W + (Z - 1 - z) * 2 + k, b)

    def send_to_row(ref, at, places):
        for to_z in places:
            for to_k in (1, 0):
                @pl.when((z != to_z) | (k != to_k))
                def _():
                    pltpu.make_async_remote_copy(
                        src_ref=ref.at[j], dst_ref=ref.at[j], send_sem=send_sem.at[0], recv_sem=recv_sem.at[at],
                        device_id=dev(y * W + to_z * 2 + to_k, b), device_id_type=MESH).start()

    places = near_first(Z)
    send_to_row(qbuf, 0, [p for p in places if p < half])

    square = (K, K)
    unit = (lax.broadcasted_iota(jnp.int32, square, 0) == lax.broadcasted_iota(jnp.int32, square, 1)).astype(F32)
    down = jnp.concatenate([unit, path.T], axis=0)[None]
    for h in (2, 1, 0):
        m = L0 >> h
        down = jnp.broadcast_to(down[:, None], (m // 2, 2, 2 * K, K)).reshape(m, 2 * K, K)
        down = bmm_t(down, transfer[0, FIRST[h]:FIRST[h] + m])
    down = bmm_t(down, basis[0])
    for l in range(0, L0, 2):
        joined = jnp.concatenate([down[l], down[l + 1]], axis=1)
        hi = joined.astype(jnp.bfloat16)
        pg_hi[:, K * l:K * (l + 2)] = hi
        pg_lo[:, K * l:K * (l + 2)] = (joined - hi.astype(F32)).astype(jnp.bfloat16)

    halo_next = (
        (leaves.at[pl.ds(L0, NEAR)], leaves.at[pl.ds(0, NEAR)], nxt),
        (tiers.at[pl.ds(NODES, NODES)], tiers.at[pl.ds(0, NODES)], nxt),
    )
    halo_previous = (
        (leaves.at[pl.ds(NEAR, NEAR)], leaves.at[pl.ds(NEAR + L0, NEAR)], prv),
        (tiers.at[pl.ds(NODES, NODES)], tiers.at[pl.ds(2 * NODES, NODES)], prv),
    )

    def send_halo(parts):
        for src, dst, to in parts:
            pltpu.make_async_remote_copy(
                src_ref=src, dst_ref=dst, send_sem=send_sem.at[1], recv_sem=recv_sem.at[2],
                device_id=to, device_id_type=MESH).start()

    send_to_row(rows, 1, [p for p in places if p < half])

    @pl.when(final)
    def _():
        send_halo(halo_next)

    @pl.when(first)
    def _():
        pl.semaphore_wait(state.at[1], 2 * half + one(origin))
        for a in (1, Y - 1):
            pl.semaphore_signal(state.at[2], inc=1, device_id=y_dev(a), device_id_type=MESH)

    @pl.when(second)
    def _():
        pl.semaphore_wait(state.at[3], 1)

    send_to_row(rows, 1, [p for p in places if p >= half])
    @pl.when(jnp.logical_not(final))
    def _():
        send_halo(halo_next)

    send_halo(halo_previous)

    for load in later:
        load.wait()

    path_y = ct[0, R, side[R]]
    for c in range(R + 1, COARSE):
        path_y = mm(path_y, ct[0, c, side[c]])
    for s in range(X - 1):
        sbuf[s] = mm_t(bc[0, s], path_y)
    if R == COARSE - 3:
        for n in range(2):
            sbuf[X - 1 + n] = mm_t(mm(ct[0, R, n], opp[0]), ct[0, R, side[R]])


    @pl.when(first)
    def _():
        for s in range(X - 1):
            far_hi[s], far_lo[s] = split(mm(sbuf[s], (pg_hi[K:], pg_lo[K:])))
        await_all(recv_sem.at[0], qbuf.at[pl.ds(1, W - 1)])
        total = qbuf[0]
        for n in range(1, W):
            total = total + qbuf[n]
        u_row = unpack(total)
        xsrc[...] = pack(mm(u_row, path_y))
        u4buf[y] = total
        pl.semaphore_wait(state.at[0], len(order_x))
        for to_x, to_y in order_xy:
            @pl.when(b != to_x)
            def _():
                pltpu.make_async_remote_copy(
                    src_ref=xsrc, dst_ref=xbuf.at[((b - to_x + X) % X) * Y + y], send_sem=send_sem.at[2],
                    recv_sem=recv_sem.at[5], device_id=dev(to_y * W + j, to_x), device_id_type=MESH).start()

            @pl.when((b == to_x) & (y != to_y))
            def _():
                pltpu.make_async_remote_copy(
                    src_ref=u4buf.at[y], dst_ref=u4buf.at[y], send_sem=send_sem.at[2], recv_sem=recv_sem.at[4],
                    device_id=dev(to_y * W + j, b), device_id_type=MESH).start()
        pl.semaphore_wait(state.at[2], 2)
        pl.semaphore_signal(state.at[3], inc=1, device_id=mate, device_id_type=MESH)

    await_all(recv_sem.at[1], rows.at[pl.ds(0, W - 1)])
    tier = unpack(rows[0:W])
    for c in range(R - 1):
        m = W >> c
        pairs = tier.reshape(m // 2, 2, RHS, K)
        left = mm(pairs[:, 0].reshape(m // 2 * RHS, K), ct[0, c, 0])
        right = mm(pairs[:, 1].reshape(m // 2 * RHS, K), ct[0, c, 1])
        tier = (left + right).reshape(m // 2, RHS, K)
        rows[START[c + 1]:START[c + 1] + m // 2] = pack(tier)

    given = None
    for c in range(R - 1, -1, -1):
        m = W >> c
        if given is None:
            given = [jnp.zeros((RHS, K), F32)] * 3
        else:
            moved = mm_t(jnp.concatenate(given, axis=0), ct[0, c, side[c]])
            given = [moved[RHS * n:RHS * (n + 1)] for n in range(3)]
        third = 3 - 6 * side[c]
        for offset, slot in ((-2, 1), (2, 2), (third, 3 - 3 * side[c])):
            at = j // (1 << c) + offset
            term = mm(unpack(rows[START[c] + (at + m) % m]), cc[0, c, slot])
            for n, keep in enumerate((at >= m, (at >= 0) & (at < m), at < 0)):
                given[n] = given[n] + jnp.where(keep, term, 0.0)
    v_own = given[1]
    gbuf[0] = pack(given[0])
    gbuf[1] = pack(given[2])
    for n, to in enumerate((y_dev(Y - 1), y_dev(1))):
        copy = pltpu.make_async_remote_copy(
            src_ref=gbuf.at[n], dst_ref=gbuf.at[2 + n], send_sem=send_sem.at[1], recv_sem=recv_sem.at[3],
            device_id=to, device_id_type=MESH)
        copy.start()

    await_all(recv_sem.at[2], tiers.at[pl.ds(0, 2 * NEAR + 2 * NODES)])
    for l in range(L0):
        total = None
        for s in range(3):
            term = mm(unpack(leaves[near_list[s, 0, l] + l]), near[0, l, s])
            total = term if total is None else total + term
        acc[l] = total

    coupled = []
    for h in range(3):
        m = L0 >> h
        terms = []
        for n in range(m):
            node = FIRST[h] + n
            total = None
            for s in range(3):
                e = coupling_list[s, 0, node]
                where = (e // m) * NODES + FIRST[h] + e % m
                term = mm(unpack(tiers[where]), coupling[0, node, s])
                total = term if total is None else total + term
            terms.append(total)
        coupled.append(jnp.stack(terms, axis=0))

    local = coupled[2]
    for h in (1, 0):
        m = L0 >> h
        local = jnp.broadcast_to(local[:, None], (m // 2, 2, RHS, K)).reshape(m, RHS, K)
        local = coupled[h] + bmm_t(local, transfer[0, FIRST[h]:FIRST[h] + m])
    field = bmm_t(local, basis[0]) + acc[...]
    for l in range(0, L0, 2):
        out_ref[0, :, K * l:K * (l + 2)] = jnp.concatenate([field[l], field[l + 1]], axis=1)

    await_all(recv_sem.at[3], gbuf.at[pl.ds(2, 2)])
    v_own = v_own + unpack(gbuf[2]) + unpack(gbuf[3])

    def finish(row):
        late = mm(jnp.concatenate([v_own, row], axis=1), (pg_hi[...], pg_lo[...]))
        out_ref[0] = out_ref[0] + late

    @pl.when(first)
    def _():
        await_all(recv_sem.at[4], u4buf.at[pl.ds(0, Y - 1)])
        if R == COARSE - 3:
            third = 3 - 6 * side[R]
            row = None
            for offset, slot in ((-2, 1), (2, 2), (third, 3 - 3 * side[R])):
                term = mm(unpack(u4buf[(y + offset + Y) % Y]), cc[0, R, slot])
                row = term if row is None else row + term
            pair = 2 * ((y // 2 + 2) % (Y // 2))
            row = row + mm(unpack(u4buf[pair]), sbuf[X - 1]) + mm(unpack(u4buf[pair + 1]), sbuf[X])
        else:
            row = mm(unpack(u4buf[(y + 2) % Y]), opp[0])

        finish(row)

        await_all(recv_sem.at[5], xbuf.at[pl.ds(Y, (X - 1) * Y)])
        bodies = []
        for s in range(X - 1):
            total = xbuf[(s + 1) * Y]
            for n in range(1, Y):
                total = total + xbuf[(s + 1) * Y + n]
            bodies.append(unpack(total))
        late = None
        for s in range(X - 1):
            term = mm(bodies[s], (far_hi[s], far_lo[s]))
            late = term if late is None else late + term
        out_ref[0] = out_ref[0] + late

        @pl.when(z == half - 1)
        def _():
            whole = row
            for s in range(X - 1):
                whole = whole + mm(bodies[s], sbuf[s])
            vbuf[...] = pack(whole)
            for to_z in range(Z - 1, half - 1, -1):
                pltpu.make_async_remote_copy(
                    src_ref=vbuf, dst_ref=vbuf, send_sem=send_sem.at[3], recv_sem=recv_sem.at[6],
                    device_id=dev(y * W + to_z * 2 + k, b), device_id_type=MESH).start()
            await_all(send_sem.at[3], xbuf.at[pl.ds(0, Z - half)])

        await_all(send_sem.at[0], xbuf.at[pl.ds(0, 2 * half - 1 + W - 1)])
        await_all(send_sem.at[2], xbuf.at[pl.ds(0, Y - 1 + (X - 1) * Y)])

    @pl.when(second)
    def _():
        await_all(recv_sem.at[6], vbuf)
        finish(unpack(vbuf[...]))
        await_all(send_sem.at[0], xbuf.at[pl.ds(0, 2 * half + W - 1)])

    await_all(send_sem.at[1], tiers.at[pl.ds(0, 2 * NEAR + 2 * NODES + 2)])


def per_device(Y, Z, X, charges, leaf_basis, near_blocks, near_list, local_transfer, local_coupling, coupling_list,
               coarse_transfer, coarse_coupling, opposite_coupling, body_coupling):
    near_at = near_list.transpose(2, 0, 1)
    coupling_at = coupling_list.transpose(2, 0, 1)
    W = 2 * Z
    R = Z.bit_length()
    dma = pltpu.SemaphoreType.DMA
    vm = lambda *shape: pltpu.VMEM(shape, F32)
    operands = (charges, leaf_basis, near_blocks, local_transfer, local_coupling,
                coarse_transfer, coarse_coupling, opposite_coupling, body_coupling)
    return pl.pallas_call(
        functools.partial(kernel, Y, Z, X),
        out_shape=pltpu.VMEM(charges.shape, F32),
        in_specs=[pl.BlockSpec(memory_space=pltpu.HBM)] * 11,
        out_specs=pl.BlockSpec(memory_space=pltpu.VMEM),
        scratch_shapes=[
            *[vm(*a.shape) for a in operands[:3]], vm(1, NODES + R, K, K), *[vm(*a.shape) for a in operands[4:]],
            pltpu.SMEM(near_at.shape, jnp.int32), pltpu.SMEM(coupling_at.shape, jnp.int32),
            vm(W, 8, 128), vm(2 * W - 2, 8, 128), vm(Y, 8, 128), vm(8, 128), vm(X * Y, 8, 128), vm(4, 8, 128), vm(X + 1, K, K),
            vm(3 * NODES, 8, 128), vm(L0 + 2 * NEAR, 8, 128),
            *[pltpu.VMEM((2 * K, L0 * K), jnp.bfloat16)] * 2, *[pltpu.VMEM((X - 1, K, L0 * K), jnp.bfloat16)] * 2, vm(L0, RHS, K),
            vm(8, 128), dma((11,)), pltpu.SemaphoreType.REGULAR((4,)), dma((4,)), dma((7,)),
        ],
        compiler_params=pltpu.CompilerParams(collective_id=0, has_side_effects=True),
    )(near_at, coupling_at, *operands)


def solution(mesh):
    n = mesh.shape["leaf"]
    Z = 8 if n == 128 else 2
    Y = n // (2 * Z)
    X = mesh.shape["top"]
    in_specs = (
        P("top", None, "leaf"),
        P("top", "leaf", None, None),
        P("top", "leaf", None, None, None),
        P("top", "leaf", None),
        P("top", "leaf", None, None),
        P("top", "leaf", None, None, None),
        P("top", "leaf", None),
        P("top", None, None, None, None),
        P("top", None, None, None, None),
        P("top", None, None),
        P("top", None, None, None),
    )
    return jax.shard_map(
        functools.partial(per_device, Y, Z, X), mesh=mesh, in_specs=in_specs,
        out_specs=P("top", None, "leaf"), check_vma=False
    )
```

```python
import functools

import jax
import jax.numpy as jnp
from jax import lax
from jax.experimental import pallas as pl
from jax.experimental.pallas import tpu as pltpu
from jax.sharding import PartitionSpec as P

HIGH = lax.Precision.HIGH
MESH = pl.DeviceIdType.MESH
F32 = jnp.float32
K = 64
RHS = 16
NEAR = 4
L0 = 8
NODES = 14
FIRST = (0, 8, 12)


def split(a):
    hi = a.astype(jnp.bfloat16)
    return hi, (a - hi.astype(F32)).astype(jnp.bfloat16)


def product(x, w, dims):
    rows = x.ndim - 2
    xh, xl = split(x)
    wh, wl = w if isinstance(w, tuple) else split(w)
    dot = functools.partial(lax.dot_general, dimension_numbers=dims, preferred_element_type=F32)
    both = dot(jnp.concatenate([xh, xl], axis=rows), wh)
    m = x.shape[rows]
    return lax.slice_in_dim(both, 0, m, axis=rows) + (lax.slice_in_dim(both, m, 2 * m, axis=rows) + dot(xh, wl))


def mm(x, w):
    return product(x, w, (((1,), (0,)), ((), ())))


def mm_t(x, w):
    return product(x, w, (((1,), (1,)), ((), ())))


def bmm(x, w):
    return product(x, w, (((2,), (1,)), ((0,), (0,))))


def bmm_t(x, w):
    return product(x, w, (((2,), (2,)), ((0,), (0,))))


def pack(x):
    h = RHS // 2
    if x.ndim == 2:
        return jnp.concatenate([x[:h], x[h:]], axis=1)
    return jnp.concatenate([x[:, :h], x[:, h:]], axis=2)


def unpack(x):
    if x.ndim == 2:
        return jnp.concatenate([x[:, :K], x[:, K:]], axis=0)
    return jnp.concatenate([x[:, :, :K], x[:, :, K:]], axis=1)


def kernel(
    Y, Z, X,
    near_list_hbm, coupling_list_hbm,
    charges_hbm, basis_hbm, near_hbm, transfer_hbm, coupling_hbm,
    ct_hbm, cc_hbm, opp_hbm, bc_hbm,
    out_ref,
    charges, basis, near, transfer, coupling, ct, cc, opp, bc, near_list, coupling_list,
    qbuf, rows, u4buf, xsrc, xbuf, gbuf, sbuf, tiers, leaves, pg_hi, pg_lo, far_hi, far_lo, acc,
    vbuf, load_sem, state, send_sem, recv_sem,
):
    ZL = Z.bit_length() - 1
    YL = Y.bit_length() - 1
    R = ZL + 1
    COARSE = R + YL
    W = 2 * Z
    N = Y * W
    START = [2 * W - (2 * W >> c) for c in range(R)]
    TILES = 2 * W - 2

    i = lax.axis_index("leaf")
    b = lax.axis_index("top")
    k = i % 2
    z = (i // 2) % Z
    y = i // W
    j = i % W
    half = Z // 2
    first = z < half
    second = z >= half
    origin = (z == 0) & (k == 0)
    final = (z == Z - 1) & (k == 1)
    one = lambda flag: jnp.where(flag, 1, 0)
    side = [(i // (1 << c)) % 2 for c in range(COARSE)]

    def dev(leaf, top):
        return {"leaf": leaf, "top": top}

    order = []
    for a in range(Z // 2, 0, -1):
        order.append(a)
        if Z - a != a:
            order.append(Z - a)
    order_y = []
    for a in range(Y // 2, 0, -1):
        order_y.append(a)
        if Y - a != a:
            order_y.append(Y - a)
    order_x = sorted(range(1, X), key=lambda a: -min(a, X - a))
    near_first = lambda count: sorted(range(count), key=lambda a: min(a, count - a))
    order_xy = [(x, r) for r in near_first(Y) for x in near_first(X)]
    order_xy.sort(key=lambda t: min(t[0], X - t[0]) + min(t[1], Y - t[1]))
    row_offsets = [(dz, dk) for dz in order for dk in (0, 1)] + [(0, 1)]

    def row_dev(dz, dk):
        return dev(y * W + ((z + dz) % Z) * 2 + (k + dk) % 2, b)

    def y_dev(dy):
        return dev(((y + dy) % Y) * W + j, b)

    def x_dev(dx):
        return dev(i, (b + dx) % X)

    nxt = dev((i + 1) % N, b)
    prv = dev((i + N - 1) % N, b)

    early = [(charges_hbm, charges), (basis_hbm, basis), (transfer_hbm.at[0], transfer.at[0, pl.ds(0, NODES)])]
    later = [
        (ct_hbm, ct), (bc_hbm, bc), (opp_hbm, opp), (cc_hbm, cc), (near_hbm, near), (coupling_hbm, coupling),
        (near_list_hbm, near_list), (coupling_list_hbm, coupling_list),
    ]
    loads = [pltpu.make_async_copy(src, dst, load_sem.at[n]) for n, (src, dst) in enumerate(early + later)]
    early, later = loads[:len(early)], loads[len(early):]
    for load in early:
        load.start()
    for c in range(R):
        pltpu.make_async_copy(ct_hbm.at[0, c, side[c]], transfer.at[0, NODES + c], load_sem.at[2]).start()

    def await_all(sem, ref):
        pltpu.make_async_copy(ref, ref, sem).wait()

    barrier = pltpu.get_barrier_semaphore()
    partners = [(min(dz, Z - dz), row_dev(dz, dk)) for dz, dk in row_offsets] + [(min(a, Y - a), y_dev(a)) for a in order_y]
    partners += [(min(a, X - a), x_dev(a)) for a in order_x]
    partners = [p for _, p in sorted(partners, key=lambda t: -t[0])]

    @pl.when(first)
    def _():
        for p in partners:
            pl.semaphore_signal(barrier, inc=1, device_id=p, device_id_type=MESH)

    @pl.when(origin)
    def _():
        pl.semaphore_signal(barrier, inc=1, device_id=prv, device_id_type=MESH)

    for load in early[:2]:
        load.wait()

    dens = charges[0]
    blocks = jnp.stack([dens[:, K * l:K * (l + 1)] for l in range(L0)], axis=0)
    leaves[NEAR:NEAR + L0] = pack(blocks)
    c0 = bmm(blocks, basis[0])
    pltpu.make_async_copy(transfer, transfer, load_sem.at[2]).wait()
    for load in later:
        load.start()
    parts = [transfer[0, NODES + c] for c in range(R)]
    while len(parts) > 1:
        parts = [mm(*parts[n:n + 2]) if n + 1 < len(parts) else parts[n] for n in range(0, len(parts), 2)]
    path = parts[0]
    up = [c0]
    for h in range(2):
        m = L0 >> h
        moved = bmm(up[-1], transfer[0, FIRST[h]:FIRST[h] + m])
        moved = moved.reshape(m // 2, 2, RHS, K)
        up.append(moved[:, 0] + moved[:, 1])
    last = [transfer[0, FIRST[2] + n] for n in range(2)]
    q_own = mm(up[2][0], mm(last[0], path)) + mm(up[2][1], mm(last[1], path))
    own = mm(up[2][0], last[0]) + mm(up[2][1], last[1])

    qbuf[j] = pack(q_own)
    rows[j] = pack(own)
    tiers[NODES:NODES + L0] = pack(up[0])
    tiers[NODES + 8:NODES + 12] = pack(up[1])
    tiers[NODES + 12:NODES + 14] = pack(up[2])

    pl.semaphore_wait(barrier, 2 * half + one(final) + one(first) * (len(order_y) + len(order_x) - 1))

    @pl.when(first)
    def _():
        for a in order_x:
            pl.semaphore_signal(state.at[0], inc=1, device_id=x_dev(a), device_id_type=MESH)

    @pl.when(second)
    def _():
        for to_z in range(half):
            for to_k in range(2):
                pl.semaphore_signal(state.at[1], inc=1, device_id=dev(y * W + to_z * 2 + to_k, b), device_id_type=MESH)

    @pl.when(final)
    def _():
        pl.semaphore_signal(state.at[1], inc=1, device_id=nxt, device_id_type=MESH)

    mate = dev(y * W + (Z - 1 - z) * 2 + k, b)

    def send_to_row(ref, at, places):
        for to_z in places:
            for to_k in (1, 0):
                @pl.when((z != to_z) | (k != to_k))
                def _():
                    pltpu.make_async_remote_copy(
                        src_ref=ref.at[j], dst_ref=ref.at[j], send_sem=send_sem.at[0], recv_sem=recv_sem.at[at],
                        device_id=dev(y * W + to_z * 2 + to_k, b), device_id_type=MESH).start()

    places = near_first(Z)
    send_to_row(qbuf, 0, [p for p in places if p < half])

    square = (K, K)
    unit = (lax.broadcasted_iota(jnp.int32, square, 0) == lax.broadcasted_iota(jnp.int32, square, 1)).astype(F32)
    down = jnp.concatenate([unit, path.T], axis=0)[None]
    for h in (2, 1, 0):
        m = L0 >> h
        down = jnp.broadcast_to(down[:, None], (m // 2, 2, 2 * K, K)).reshape(m, 2 * K, K)
        down = bmm_t(down, transfer[0, FIRST[h]:FIRST[h] + m])
    down = bmm_t(down, basis[0])
    for l in range(0, L0, 2):
        joined = jnp.concatenate([down[l], down[l + 1]], axis=1)
        hi = joined.astype(jnp.bfloat16)
        pg_hi[:, K * l:K * (l + 2)] = hi
        pg_lo[:, K * l:K * (l + 2)] = (joined - hi.astype(F32)).astype(jnp.bfloat16)

    for load in later:
        load.wait()

    path_y = ct[0, R, side[R]]
    for c in range(R + 1, COARSE):
        path_y = mm(path_y, ct[0, c, side[c]])
    for s in range(X - 1):
        sbuf[s] = mm_t(bc[0, s], path_y)
    if R == COARSE - 3:
        for n in range(2):
            sbuf[X - 1 + n] = mm_t(mm(ct[0, R, n], opp[0]), ct[0, R, side[R]])


    halo_next = (
        (leaves.at[pl.ds(L0, NEAR)], leaves.at[pl.ds(0, NEAR)], nxt),
        (tiers.at[pl.ds(NODES, NODES)], tiers.at[pl.ds(0, NODES)], nxt),
    )
    halo_previous = (
        (leaves.at[pl.ds(NEAR, NEAR)], leaves.at[pl.ds(NEAR + L0, NEAR)], prv),
        (tiers.at[pl.ds(NODES, NODES)], tiers.at[pl.ds(2 * NODES, NODES)], prv),
    )

    def send_halo(parts):
        for src, dst, to in parts:
            pltpu.make_async_remote_copy(
                src_ref=src, dst_ref=dst, send_sem=send_sem.at[1], recv_sem=recv_sem.at[2],
                device_id=to, device_id_type=MESH).start()

    send_to_row(rows, 1, [p for p in places if p < half])

    @pl.when(first)
    def _():
        pl.semaphore_wait(state.at[1], 2 * half + one(origin))
        for a in (1, Y - 1):
            pl.semaphore_signal(state.at[2], inc=1, device_id=y_dev(a), device_id_type=MESH)

    @pl.when(second)
    def _():
        pl.semaphore_wait(state.at[3], 1)

    send_to_row(rows, 1, [p for p in places if p >= half])
    send_halo(halo_next + halo_previous)

    @pl.when(first)
    def _():
        for s in range(X - 1):
            far_hi[s], far_lo[s] = split(mm(sbuf[s], (pg_hi[K:], pg_lo[K:])))
        pl.semaphore_wait(state.at[2], 2)
        pl.semaphore_signal(state.at[3], inc=1, device_id=mate, device_id_type=MESH)
        await_all(recv_sem.at[0], qbuf.at[pl.ds(1, W - 1)])
        total = qbuf[0]
        for n in range(1, W):
            total = total + qbuf[n]
        u_row = unpack(total)
        xsrc[...] = pack(mm(u_row, path_y))
        u4buf[y] = total
        pl.semaphore_wait(state.at[0], len(order_x))
        for to_x, to_y in order_xy:
            @pl.when(b != to_x)
            def _():
                pltpu.make_async_remote_copy(
                    src_ref=xsrc, dst_ref=xbuf.at[((b - to_x + X) % X) * Y + y], send_sem=send_sem.at[2],
                    recv_sem=recv_sem.at[5], device_id=dev(to_y * W + j, to_x), device_id_type=MESH).start()

            @pl.when((b == to_x) & (y != to_y))
            def _():
                pltpu.make_async_remote_copy(
                    src_ref=u4buf.at[y], dst_ref=u4buf.at[y], send_sem=send_sem.at[2], recv_sem=recv_sem.at[4],
                    device_id=dev(to_y * W + j, b), device_id_type=MESH).start()

    await_all(recv_sem.at[1], rows.at[pl.ds(0, W - 1)])
    tier = unpack(rows[0:W])
    for c in range(R - 1):
        m = W >> c
        pairs = tier.reshape(m // 2, 2, RHS, K)
        left = mm(pairs[:, 0].reshape(m // 2 * RHS, K), ct[0, c, 0])
        right = mm(pairs[:, 1].reshape(m // 2 * RHS, K), ct[0, c, 1])
        tier = (left + right).reshape(m // 2, RHS, K)
        rows[START[c + 1]:START[c + 1] + m // 2] = pack(tier)

    given = None
    for c in range(R - 1, -1, -1):
        m = W >> c
        if given is None:
            given = [jnp.zeros((RHS, K), F32)] * 3
        else:
            moved = mm_t(jnp.concatenate(given, axis=0), ct[0, c, side[c]])
            given = [moved[RHS * n:RHS * (n + 1)] for n in range(3)]
        third = 3 - 6 * side[c]
        for offset, slot in ((-2, 1), (2, 2), (third, 3 - 3 * side[c])):
            at = j // (1 << c) + offset
            term = mm(unpack(rows[START[c] + (at + m) % m]), cc[0, c, slot])
            for n, keep in enumerate((at >= m, (at >= 0) & (at < m), at < 0)):
                given[n] = given[n] + jnp.where(keep, term, 0.0)
    v_own = given[1]
    gbuf[0] = pack(given[0])
    gbuf[1] = pack(given[2])
    for n, to in enumerate((y_dev(Y - 1), y_dev(1))):
        copy = pltpu.make_async_remote_copy(
            src_ref=gbuf.at[n], dst_ref=gbuf.at[2 + n], send_sem=send_sem.at[1], recv_sem=recv_sem.at[3],
            device_id=to, device_id_type=MESH)
        copy.start()

    await_all(recv_sem.at[2], tiers.at[pl.ds(0, 2 * NEAR + 2 * NODES)])
    for l in range(L0):
        total = None
        for s in range(3):
            term = mm(unpack(leaves[near_list[s, 0, l] + l]), near[0, l, s])
            total = term if total is None else total + term
        acc[l] = total

    coupled = []
    for h in range(3):
        m = L0 >> h
        terms = []
        for n in range(m):
            node = FIRST[h] + n
            total = None
            for s in range(3):
                e = coupling_list[s, 0, node]
                where = (e // m) * NODES + FIRST[h] + e % m
                term = mm(unpack(tiers[where]), coupling[0, node, s])
                total = term if total is None else total + term
            terms.append(total)
        coupled.append(jnp.stack(terms, axis=0))

    local = coupled[2]
    for h in (1, 0):
        m = L0 >> h
        local = jnp.broadcast_to(local[:, None], (m // 2, 2, RHS, K)).reshape(m, RHS, K)
        local = coupled[h] + bmm_t(local, transfer[0, FIRST[h]:FIRST[h] + m])
    field = bmm_t(local, basis[0]) + acc[...]
    for l in range(0, L0, 2):
        out_ref[0, :, K * l:K * (l + 2)] = jnp.concatenate([field[l], field[l + 1]], axis=1)

    await_all(recv_sem.at[3], gbuf.at[pl.ds(2, 2)])
    v_own = v_own + unpack(gbuf[2]) + unpack(gbuf[3])

    def finish(row):
        late = mm(jnp.concatenate([v_own, row], axis=1), (pg_hi[...], pg_lo[...]))
        out_ref[0] = out_ref[0] + late

    @pl.when(first)
    def _():
        await_all(recv_sem.at[4], u4buf.at[pl.ds(0, Y - 1)])
        if R == COARSE - 3:
            third = 3 - 6 * side[R]
            row = None
            for offset, slot in ((-2, 1), (2, 2), (third, 3 - 3 * side[R])):
                term = mm(unpack(u4buf[(y + offset + Y) % Y]), cc[0, R, slot])
                row = term if row is None else row + term
            pair = 2 * ((y // 2 + 2) % (Y // 2))
            row = row + mm(unpack(u4buf[pair]), sbuf[X - 1]) + mm(unpack(u4buf[pair + 1]), sbuf[X])
        else:
            row = mm(unpack(u4buf[(y + 2) % Y]), opp[0])

        finish(row)

        await_all(recv_sem.at[5], xbuf.at[pl.ds(Y, (X - 1) * Y)])
        bodies = []
        for s in range(X - 1):
            total = xbuf[(s + 1) * Y]
            for n in range(1, Y):
                total = total + xbuf[(s + 1) * Y + n]
            bodies.append(unpack(total))
        late = None
        for s in range(X - 1):
            term = mm(bodies[s], (far_hi[s], far_lo[s]))
            late = term if late is None else late + term
        out_ref[0] = out_ref[0] + late

        @pl.when(z == half - 1)
        def _():
            whole = row
            for s in range(X - 1):
                whole = whole + mm(bodies[s], sbuf[s])
            vbuf[...] = pack(whole)
            for to_z in range(Z - 1, half - 1, -1):
                pltpu.make_async_remote_copy(
                    src_ref=vbuf, dst_ref=vbuf, send_sem=send_sem.at[3], recv_sem=recv_sem.at[6],
                    device_id=dev(y * W + to_z * 2 + k, b), device_id_type=MESH).start()
            await_all(send_sem.at[3], xbuf.at[pl.ds(0, Z - half)])

        await_all(send_sem.at[0], xbuf.at[pl.ds(0, 2 * half - 1 + W - 1)])
        await_all(send_sem.at[2], xbuf.at[pl.ds(0, Y - 1 + (X - 1) * Y)])

    @pl.when(second)
    def _():
        await_all(recv_sem.at[6], vbuf)
        finish(unpack(vbuf[...]))
        await_all(send_sem.at[0], xbuf.at[pl.ds(0, 2 * half + W - 1)])

    await_all(send_sem.at[1], tiers.at[pl.ds(0, 2 * NEAR + 2 * NODES + 2)])


def per_device(Y, Z, X, charges, leaf_basis, near_blocks, near_list, local_transfer, local_coupling, coupling_list,
               coarse_transfer, coarse_coupling, opposite_coupling, body_coupling):
    near_at = near_list.transpose(2, 0, 1)
    coupling_at = coupling_list.transpose(2, 0, 1)
    W = 2 * Z
    R = Z.bit_length()
    dma = pltpu.SemaphoreType.DMA
    vm = lambda *shape: pltpu.VMEM(shape, F32)
    operands = (charges, leaf_basis, near_blocks, local_transfer, local_coupling,
                coarse_transfer, coarse_coupling, opposite_coupling, body_coupling)
    return pl.pallas_call(
        functools.partial(kernel, Y, Z, X),
        out_shape=pltpu.VMEM(charges.shape, F32),
        in_specs=[pl.BlockSpec(memory_space=pltpu.HBM)] * 11,
        out_specs=pl.BlockSpec(memory_space=pltpu.VMEM),
        scratch_shapes=[
            *[vm(*a.shape) for a in operands[:3]], vm(1, NODES + R, K, K), *[vm(*a.shape) for a in operands[4:]],
            pltpu.SMEM(near_at.shape, jnp.int32), pltpu.SMEM(coupling_at.shape, jnp.int32),
            vm(W, 8, 128), vm(2 * W - 2, 8, 128), vm(Y, 8, 128), vm(8, 128), vm(X * Y, 8, 128), vm(4, 8, 128), vm(X + 1, K, K),
            vm(3 * NODES, 8, 128), vm(L0 + 2 * NEAR, 8, 128),
            *[pltpu.VMEM((2 * K, L0 * K), jnp.bfloat16)] * 2, *[pltpu.VMEM((X - 1, K, L0 * K), jnp.bfloat16)] * 2, vm(L0, RHS, K),
            vm(8, 128), dma((11,)), pltpu.SemaphoreType.REGULAR((4,)), dma((4,)), dma((7,)),
        ],
        compiler_params=pltpu.CompilerParams(collective_id=0, has_side_effects=True),
    )(near_at, coupling_at, *operands)


def solution(mesh):
    n = mesh.shape["leaf"]
    Z = 8 if n == 128 else 2
    Y = n // (2 * Z)
    X = mesh.shape["top"]
    in_specs = (
        P("top", None, "leaf"),
        P("top", "leaf", None, None),
        P("top", "leaf", None, None, None),
        P("top", "leaf", None),
        P("top", "leaf", None, None),
        P("top", "leaf", None, None, None),
        P("top", "leaf", None),
        P("top", None, None, None, None),
        P("top", None, None, None, None),
        P("top", None, None),
        P("top", None, None, None),
    )
    return jax.shard_map(
        functools.partial(per_device, Y, Z, X), mesh=mesh, in_specs=in_specs,
        out_specs=P("top", None, "leaf"), check_vma=False
    )
```

```python
import functools

import jax
import jax.numpy as jnp
from jax import lax
from jax.experimental import pallas as pl
from jax.experimental.pallas import tpu as pltpu
from jax.sharding import PartitionSpec as P

HIGH = lax.Precision.HIGH
MESH = pl.DeviceIdType.MESH
F32 = jnp.float32
K = 64
RHS = 16
NEAR = 4
L0 = 8
NODES = 14
FIRST = (0, 8, 12)


def split(a):
    hi = a.astype(jnp.bfloat16)
    return hi, (a - hi.astype(F32)).astype(jnp.bfloat16)


def product(x, w, dims):
    rows = x.ndim - 2
    xh, xl = split(x)
    wh, wl = w if isinstance(w, tuple) else split(w)
    dot = functools.partial(lax.dot_general, dimension_numbers=dims, preferred_element_type=F32)
    both = dot(jnp.concatenate([xh, xl], axis=rows), wh)
    m = x.shape[rows]
    return lax.slice_in_dim(both, 0, m, axis=rows) + (lax.slice_in_dim(both, m, 2 * m, axis=rows) + dot(xh, wl))


def mm(x, w):
    return product(x, w, (((1,), (0,)), ((), ())))


def mm_t(x, w):
    return product(x, w, (((1,), (1,)), ((), ())))


def bmm(x, w):
    return product(x, w, (((2,), (1,)), ((0,), (0,))))


def bmm_t(x, w):
    return product(x, w, (((2,), (2,)), ((0,), (0,))))


def pack(x):
    h = RHS // 2
    if x.ndim == 2:
        return jnp.concatenate([x[:h], x[h:]], axis=1)
    return jnp.concatenate([x[:, :h], x[:, h:]], axis=2)


def unpack(x):
    if x.ndim == 2:
        return jnp.concatenate([x[:, :K], x[:, K:]], axis=0)
    return jnp.concatenate([x[:, :, :K], x[:, :, K:]], axis=1)


def kernel(
    Y, Z, X,
    near_list_hbm, coupling_list_hbm,
    charges_hbm, basis_hbm, near_hbm, transfer_hbm, coupling_hbm,
    ct_hbm, cc_hbm, opp_hbm, bc_hbm,
    out_ref,
    charges, basis, near, transfer, coupling, ct, cc, opp, bc, near_list, coupling_list,
    qbuf, rows, u4buf, xsrc, xbuf, gbuf, sbuf, tiers, leaves, pg_hi, pg_lo, far_hi, far_lo, acc,
    vbuf, load_sem, state, send_sem, recv_sem,
):
    ZL = Z.bit_length() - 1
    YL = Y.bit_length() - 1
    R = ZL + 1
    COARSE = R + YL
    W = 2 * Z
    N = Y * W
    START = [2 * W - (2 * W >> c) for c in range(R)]
    TILES = 2 * W - 2

    i = lax.axis_index("leaf")
    b = lax.axis_index("top")
    k = i % 2
    z = (i // 2) % Z
    y = i // W
    j = i % W
    half = Z // 2
    first = z < half
    second = z >= half
    origin = (z == 0) & (k == 0)
    final = (z == Z - 1) & (k == 1)
    one = lambda flag: jnp.where(flag, 1, 0)
    side = [(i // (1 << c)) % 2 for c in range(COARSE)]

    def dev(leaf, top):
        return {"leaf": leaf, "top": top}

    order = []
    for a in range(Z // 2, 0, -1):
        order.append(a)
        if Z - a != a:
            order.append(Z - a)
    order_y = []
    for a in range(Y // 2, 0, -1):
        order_y.append(a)
        if Y - a != a:
            order_y.append(Y - a)
    order_x = sorted(range(1, X), key=lambda a: -min(a, X - a))
    near_first = lambda count: sorted(range(count), key=lambda a: min(a, count - a))
    order_xy = [(x, r) for r in near_first(Y) for x in near_first(X)]
    order_xy.sort(key=lambda t: min(t[0], X - t[0]) + min(t[1], Y - t[1]))
    row_offsets = [(dz, dk) for dz in order for dk in (0, 1)] + [(0, 1)]

    def row_dev(dz, dk):
        return dev(y * W + ((z + dz) % Z) * 2 + (k + dk) % 2, b)

    def y_dev(dy):
        return dev(((y + dy) % Y) * W + j, b)

    def x_dev(dx):
        return dev(i, (b + dx) % X)

    nxt = dev((i + 1) % N, b)
    prv = dev((i + N - 1) % N, b)

    early = [(charges_hbm, charges), (basis_hbm, basis), (transfer_hbm.at[0], transfer.at[0, pl.ds(0, NODES)])]
    later = [
        (cc_hbm, cc), (coupling_hbm, coupling), (near_list_hbm, near_list), (coupling_list_hbm, coupling_list),
    ]
    loads = [pltpu.make_async_copy(src, dst, load_sem.at[n]) for n, (src, dst) in enumerate(early + later)]
    early, later = loads[:len(early)], loads[len(early):]
    for load in early:
        load.start()
    for c in range(R):
        pltpu.make_async_copy(ct_hbm.at[0, c, side[c]], transfer.at[0, NODES + c], load_sem.at[2]).start()

    def await_all(sem, ref):
        pltpu.make_async_copy(ref, ref, sem).wait()

    barrier = pltpu.get_barrier_semaphore()
    partners = [(min(dz, Z - dz), row_dev(dz, dk)) for dz, dk in row_offsets] + [(min(a, Y - a), y_dev(a)) for a in order_y]
    partners += [(min(a, X - a), x_dev(a)) for a in order_x]
    partners = [p for _, p in sorted(partners, key=lambda t: -t[0])]

    @pl.when(first)
    def _():
        for p in partners:
            pl.semaphore_signal(barrier, inc=1, device_id=p, device_id_type=MESH)

    @pl.when(origin)
    def _():
        pl.semaphore_signal(barrier, inc=1, device_id=prv, device_id_type=MESH)

    for load in early[:2]:
        load.wait()

    @pl.when(second)
    def _():
        pl.semaphore_wait(barrier, 2 * half + one(final))
        for to_z in range(half):
            for to_k in range(2):
                pl.semaphore_signal(state.at[1], inc=1, device_id=dev(y * W + to_z * 2 + to_k, b), device_id_type=MESH)

    @pl.when(final)
    def _():
        pl.semaphore_signal(state.at[1], inc=1, device_id=nxt, device_id_type=MESH)

    dens = charges[0]
    blocks = jnp.stack([dens[:, K * l:K * (l + 1)] for l in range(L0)], axis=0)
    leaves[NEAR:NEAR + L0] = pack(blocks)
    c0 = bmm(blocks, basis[0])
    pltpu.make_async_copy(transfer, transfer, load_sem.at[2]).wait()
    for load in later:
        load.start()
    for src, dst in ((ct_hbm, ct), (bc_hbm, bc), (opp_hbm, opp), (near_hbm, near)):
        pltpu.make_async_copy(src, dst, load_sem.at[7]).start()
    parts = [transfer[0, NODES + c] for c in range(R)]
    while len(parts) > 1:
        parts = [mm(*parts[n:n + 2]) if n + 1 < len(parts) else parts[n] for n in range(0, len(parts), 2)]
    path = parts[0]
    up = [c0]
    for h in range(2):
        m = L0 >> h
        moved = bmm(up[-1], transfer[0, FIRST[h]:FIRST[h] + m])
        moved = moved.reshape(m // 2, 2, RHS, K)
        up.append(moved[:, 0] + moved[:, 1])
    last = [transfer[0, FIRST[2] + n] for n in range(2)]
    q_own = mm(up[2][0], mm(last[0], path)) + mm(up[2][1], mm(last[1], path))
    own = mm(up[2][0], last[0]) + mm(up[2][1], last[1])

    qbuf[j] = pack(q_own)
    rows[j] = pack(own)
    tiers[NODES:NODES + L0] = pack(up[0])
    tiers[NODES + 8:NODES + 12] = pack(up[1])
    tiers[NODES + 12:NODES + 14] = pack(up[2])

    @pl.when(first)
    def _():
        pl.semaphore_wait(barrier, 2 * half - 1 + len(order_y) + len(order_x))
        for a in order_x:
            pl.semaphore_signal(state.at[0], inc=1, device_id=x_dev(a), device_id_type=MESH)

    mate = dev(y * W + (Z - 1 - z) * 2 + k, b)

    def send_to_row(ref, at, places):
        for to_z in places:
            for to_k in (1, 0):
                @pl.when((z != to_z) | (k != to_k))
                def _():
                    pltpu.make_async_remote_copy(
                        src_ref=ref.at[j], dst_ref=ref.at[j], send_sem=send_sem.at[0], recv_sem=recv_sem.at[at],
                        device_id=dev(y * W + to_z * 2 + to_k, b), device_id_type=MESH).start()

    places = near_first(Z)
    send_to_row(qbuf, 0, [p for p in places if p < half])

    square = (K, K)
    unit = (lax.broadcasted_iota(jnp.int32, square, 0) == lax.broadcasted_iota(jnp.int32, square, 1)).astype(F32)
    down = jnp.concatenate([unit, path.T], axis=0)[None]
    for h in (2, 1, 0):
        m = L0 >> h
        down = jnp.broadcast_to(down[:, None], (m // 2, 2, 2 * K, K)).reshape(m, 2 * K, K)
        down = bmm_t(down, transfer[0, FIRST[h]:FIRST[h] + m])
    down = bmm_t(down, basis[0])
    for l in range(0, L0, 2):
        joined = jnp.concatenate([down[l], down[l + 1]], axis=1)
        hi = joined.astype(jnp.bfloat16)
        pg_hi[:, K * l:K * (l + 2)] = hi
        pg_lo[:, K * l:K * (l + 2)] = (joined - hi.astype(F32)).astype(jnp.bfloat16)

    for load in later:
        load.wait()
    await_all(load_sem.at[7], coupling)

    path_y = ct[0, R, side[R]]
    for c in range(R + 1, COARSE):
        path_y = mm(path_y, ct[0, c, side[c]])
    for s in range(X - 1):
        sbuf[s] = mm_t(bc[0, s], path_y)
    if R == COARSE - 3:
        for n in range(2):
            sbuf[X - 1 + n] = mm_t(mm(ct[0, R, n], opp[0]), ct[0, R, side[R]])


    halo_next = (
        (leaves.at[pl.ds(L0, NEAR)], leaves.at[pl.ds(0, NEAR)], nxt),
        (tiers.at[pl.ds(NODES, NODES)], tiers.at[pl.ds(0, NODES)], nxt),
    )
    halo_previous = (
        (leaves.at[pl.ds(NEAR, NEAR)], leaves.at[pl.ds(NEAR + L0, NEAR)], prv),
        (tiers.at[pl.ds(NODES, NODES)], tiers.at[pl.ds(2 * NODES, NODES)], prv),
    )

    def send_halo(parts):
        for src, dst, to in parts:
            pltpu.make_async_remote_copy(
                src_ref=src, dst_ref=dst, send_sem=send_sem.at[1], recv_sem=recv_sem.at[2],
                device_id=to, device_id_type=MESH).start()

    send_to_row(rows, 1, [p for p in places if p < half])

    @pl.when(first)
    def _():
        pl.semaphore_wait(state.at[1], 2 * half + one(origin))
        for a in (1, Y - 1):
            pl.semaphore_signal(state.at[2], inc=1, device_id=y_dev(a), device_id_type=MESH)

    @pl.when(second)
    def _():
        pl.semaphore_wait(state.at[3], 1)

    send_to_row(rows, 1, [p for p in places if p >= half])
    send_halo(halo_next + halo_previous)

    @pl.when(first)
    def _():
        for s in range(X - 1):
            far_hi[s], far_lo[s] = split(mm(sbuf[s], (pg_hi[K:], pg_lo[K:])))
        pl.semaphore_wait(state.at[2], 2)
        pl.semaphore_signal(state.at[3], inc=1, device_id=mate, device_id_type=MESH)
        await_all(recv_sem.at[0], qbuf.at[pl.ds(1, W - 1)])
        total = qbuf[0]
        for n in range(1, W):
            total = total + qbuf[n]
        u_row = unpack(total)
        xsrc[...] = pack(mm(u_row, path_y))
        u4buf[y] = total
        pl.semaphore_wait(state.at[0], len(order_x))
        for to_x, to_y in order_xy:
            @pl.when(b != to_x)
            def _():
                pltpu.make_async_remote_copy(
                    src_ref=xsrc, dst_ref=xbuf.at[((b - to_x + X) % X) * Y + y], send_sem=send_sem.at[2],
                    recv_sem=recv_sem.at[5], device_id=dev(to_y * W + j, to_x), device_id_type=MESH).start()

            @pl.when((b == to_x) & (y != to_y))
            def _():
                pltpu.make_async_remote_copy(
                    src_ref=u4buf.at[y], dst_ref=u4buf.at[y], send_sem=send_sem.at[2], recv_sem=recv_sem.at[4],
                    device_id=dev(to_y * W + j, b), device_id_type=MESH).start()

    await_all(recv_sem.at[1], rows.at[pl.ds(0, W - 1)])
    tier = unpack(rows[0:W])
    for c in range(R - 1):
        m = W >> c
        pairs = tier.reshape(m // 2, 2, RHS, K)
        left = mm(pairs[:, 0].reshape(m // 2 * RHS, K), ct[0, c, 0])
        right = mm(pairs[:, 1].reshape(m // 2 * RHS, K), ct[0, c, 1])
        tier = (left + right).reshape(m // 2, RHS, K)
        rows[START[c + 1]:START[c + 1] + m // 2] = pack(tier)

    given = None
    for c in range(R - 1, -1, -1):
        m = W >> c
        if given is None:
            given = [jnp.zeros((RHS, K), F32)] * 3
        else:
            moved = mm_t(jnp.concatenate(given, axis=0), ct[0, c, side[c]])
            given = [moved[RHS * n:RHS * (n + 1)] for n in range(3)]
        third = 3 - 6 * side[c]
        for offset, slot in ((-2, 1), (2, 2), (third, 3 - 3 * side[c])):
            at = j // (1 << c) + offset
            term = mm(unpack(rows[START[c] + (at + m) % m]), cc[0, c, slot])
            for n, keep in enumerate((at >= m, (at >= 0) & (at < m), at < 0)):
                given[n] = given[n] + jnp.where(keep, term, 0.0)
    v_own = given[1]
    gbuf[0] = pack(given[0])
    gbuf[1] = pack(given[2])
    for n, to in enumerate((y_dev(Y - 1), y_dev(1))):
        copy = pltpu.make_async_remote_copy(
            src_ref=gbuf.at[n], dst_ref=gbuf.at[2 + n], send_sem=send_sem.at[1], recv_sem=recv_sem.at[3],
            device_id=to, device_id_type=MESH)
        copy.start()

    await_all(recv_sem.at[2], tiers.at[pl.ds(0, 2 * NEAR + 2 * NODES)])
    for l in range(L0):
        total = None
        for s in range(3):
            term = mm(unpack(leaves[near_list[s, 0, l] + l]), near[0, l, s])
            total = term if total is None else total + term
        acc[l] = total

    coupled = []
    for h in range(3):
        m = L0 >> h
        terms = []
        for n in range(m):
            node = FIRST[h] + n
            total = None
            for s in range(3):
                e = coupling_list[s, 0, node]
                where = (e // m) * NODES + FIRST[h] + e % m
                term = mm(unpack(tiers[where]), coupling[0, node, s])
                total = term if total is None else total + term
            terms.append(total)
        coupled.append(jnp.stack(terms, axis=0))

    local = coupled[2]
    for h in (1, 0):
        m = L0 >> h
        local = jnp.broadcast_to(local[:, None], (m // 2, 2, RHS, K)).reshape(m, RHS, K)
        local = coupled[h] + bmm_t(local, transfer[0, FIRST[h]:FIRST[h] + m])
    field = bmm_t(local, basis[0]) + acc[...]
    for l in range(0, L0, 2):
        out_ref[0, :, K * l:K * (l + 2)] = jnp.concatenate([field[l], field[l + 1]], axis=1)

    await_all(recv_sem.at[3], gbuf.at[pl.ds(2, 2)])
    v_own = v_own + unpack(gbuf[2]) + unpack(gbuf[3])

    def finish(row):
        late = mm(jnp.concatenate([v_own, row], axis=1), (pg_hi[...], pg_lo[...]))
        out_ref[0] = out_ref[0] + late

    @pl.when(first)
    def _():
        await_all(recv_sem.at[4], u4buf.at[pl.ds(0, Y - 1)])
        if R == COARSE - 3:
            third = 3 - 6 * side[R]
            row = None
            for offset, slot in ((-2, 1), (2, 2), (third, 3 - 3 * side[R])):
                term = mm(unpack(u4buf[(y + offset + Y) % Y]), cc[0, R, slot])
                row = term if row is None else row + term
            pair = 2 * ((y // 2 + 2) % (Y // 2))
            row = row + mm(unpack(u4buf[pair]), sbuf[X - 1]) + mm(unpack(u4buf[pair + 1]), sbuf[X])
        else:
            row = mm(unpack(u4buf[(y + 2) % Y]), opp[0])

        finish(row)

        await_all(recv_sem.at[5], xbuf.at[pl.ds(Y, (X - 1) * Y)])
        bodies = []
        for s in range(X - 1):
            total = xbuf[(s + 1) * Y]
            for n in range(1, Y):
                total = total + xbuf[(s + 1) * Y + n]
            bodies.append(unpack(total))
        late = None
        for s in range(X - 1):
            term = mm(bodies[s], (far_hi[s], far_lo[s]))
            late = term if late is None else late + term
        out_ref[0] = out_ref[0] + late

        @pl.when(z == half - 1)
        def _():
            whole = row
            for s in range(X - 1):
                whole = whole + mm(bodies[s], sbuf[s])
            vbuf[...] = pack(whole)
            for to_z in range(Z - 1, half - 1, -1):
                pltpu.make_async_remote_copy(
                    src_ref=vbuf, dst_ref=vbuf, send_sem=send_sem.at[3], recv_sem=recv_sem.at[6],
                    device_id=dev(y * W + to_z * 2 + k, b), device_id_type=MESH).start()
            await_all(send_sem.at[3], xbuf.at[pl.ds(0, Z - half)])

        await_all(send_sem.at[0], xbuf.at[pl.ds(0, 2 * half - 1 + W - 1)])
        await_all(send_sem.at[2], xbuf.at[pl.ds(0, Y - 1 + (X - 1) * Y)])

    @pl.when(second)
    def _():
        await_all(recv_sem.at[6], vbuf)
        finish(unpack(vbuf[...]))
        await_all(send_sem.at[0], xbuf.at[pl.ds(0, 2 * half + W - 1)])

    await_all(send_sem.at[1], tiers.at[pl.ds(0, 2 * NEAR + 2 * NODES + 2)])


def per_device(Y, Z, X, charges, leaf_basis, near_blocks, near_list, local_transfer, local_coupling, coupling_list,
               coarse_transfer, coarse_coupling, opposite_coupling, body_coupling):
    near_at = near_list.transpose(2, 0, 1)
    coupling_at = coupling_list.transpose(2, 0, 1)
    W = 2 * Z
    R = Z.bit_length()
    dma = pltpu.SemaphoreType.DMA
    vm = lambda *shape: pltpu.VMEM(shape, F32)
    operands = (charges, leaf_basis, near_blocks, local_transfer, local_coupling,
                coarse_transfer, coarse_coupling, opposite_coupling, body_coupling)
    return pl.pallas_call(
        functools.partial(kernel, Y, Z, X),
        out_shape=pltpu.VMEM(charges.shape, F32),
        in_specs=[pl.BlockSpec(memory_space=pltpu.HBM)] * 11,
        out_specs=pl.BlockSpec(memory_space=pltpu.VMEM),
        scratch_shapes=[
            *[vm(*a.shape) for a in operands[:3]], vm(1, NODES + R, K, K), *[vm(*a.shape) for a in operands[4:]],
            pltpu.SMEM(near_at.shape, jnp.int32), pltpu.SMEM(coupling_at.shape, jnp.int32),
            vm(W, 8, 128), vm(2 * W - 2, 8, 128), vm(Y, 8, 128), vm(8, 128), vm(X * Y, 8, 128), vm(4, 8, 128), vm(X + 1, K, K),
            vm(3 * NODES, 8, 128), vm(L0 + 2 * NEAR, 8, 128),
            *[pltpu.VMEM((2 * K, L0 * K), jnp.bfloat16)] * 2, *[pltpu.VMEM((X - 1, K, L0 * K), jnp.bfloat16)] * 2, vm(L0, RHS, K),
            vm(8, 128), dma((8,)), pltpu.SemaphoreType.REGULAR((4,)), dma((4,)), dma((7,)),
        ],
        compiler_params=pltpu.CompilerParams(collective_id=0, has_side_effects=True),
    )(near_at, coupling_at, *operands)


def solution(mesh):
    n = mesh.shape["leaf"]
    Z = 8 if n == 128 else 2
    Y = n // (2 * Z)
    X = mesh.shape["top"]
    in_specs = (
        P("top", None, "leaf"),
        P("top", "leaf", None, None),
        P("top", "leaf", None, None, None),
        P("top", "leaf", None),
        P("top", "leaf", None, None),
        P("top", "leaf", None, None, None),
        P("top", "leaf", None),
        P("top", None, None, None, None),
        P("top", None, None, None, None),
        P("top", None, None),
        P("top", None, None, None),
    )
    return jax.shard_map(
        functools.partial(per_device, Y, Z, X), mesh=mesh, in_specs=in_specs,
        out_specs=P("top", None, "leaf"), check_vma=False
    )
```
